32 devices in a mesh: clip: 4 (over y, core), frame: 2 (over x), pix: 4 (over z).
Axes of the slice: x: 2, y: 2, z: 4, core: 2. Of those that a mesh axis runs over, the one named last changes fastest.
Arguments:
- features: bfloat16 [8, 8, 96, 256], P(('clip', 'frame'), 'pix'), parts along dimension 0, may hold values from -6 to 6
Outputs:
- forward_full: bfloat16 [8, 8, 96, 768], P(('clip', 'frame'), 'pix'), parts along dimension 0
- forward_half: bfloat16 [8, 8, 96, 192], P(('clip', 'frame'), 'pix'), parts along dimension 0
- forward_quarter: bfloat16 [8, 8, 96, 48], P(('clip', 'frame'), 'pix'), parts along dimension 0
- forward_eighth: bfloat16 [8, 8, 96, 12], P(('clip', 'frame'), 'pix'), parts along dimension 0
- backward_full: bfloat16 [8, 8, 96, 768], P(('clip', 'frame'), 'pix'), parts along dimension 0
- backward_half: bfloat16 [8, 8, 96, 192], P(('clip', 'frame'), 'pix'), parts along dimension 0
- backward_quarter: bfloat16 [8, 8, 96, 48], P(('clip', 'frame'), 'pix'), parts along dimension 0
- backward_eighth: bfloat16 [8, 8, 96, 12], P(('clip', 'frame'), 'pix'), parts along dimension 0
The draws below stay inside these ranges and needn't reach their ends.
There are 4 independent parts, one for each index of `clip`. The reference program is written for one: setup_inputs(seed, part) draws one part's arguments, and reference() takes and returns one part's arrays. A program takes and returns all parts, laid end to end along the dimension named above; each array names one. Nothing has to cross between parts.
All inputs are finite; a program needn't handle non-finite values.
Results may differ from the reference program's by a relative error of at most 0.001.
Values may be sent and summed in bfloat16 or wider, within the bound.
No kernel may reach another device: no remote copies, remote signals or barrier semaphores. Data moves between devices by JAX's collectives and lax.ppermute only.
A program may use at most 64 MiB of HBM per device.

```python
import math
import jax
import jax.numpy as jnp
from jax import lax

C = 256
W = 96
H = 8
FRAMES = 2


def levels(stream_key, shape, shards, low, high):
    level, own = 1.0, jax.random.fold_in(stream_key, 6)
    for dim, parts in shards:
        draws = jnp.exp(jax.random.uniform(jax.random.fold_in(own, dim), (parts,), jnp.float32, low / len(shards), high / len(shards)))
        level = level * jnp.repeat(draws, shape[dim] // parts).reshape([-1 if axis == dim else 1 for axis in range(len(shape))])
    return level


def centred(rng, shape, deviation, most, cuts=(), kind=jnp.bfloat16):
    factor_of = levels(rng, shape, cuts, -0.22, 0.18) if cuts else 1.0
    array = jax.random.normal(rng, shape, jnp.float32) * deviation * factor_of
    return jnp.minimum(jnp.maximum(array, -most), most).astype(kind)


def setup_inputs(seed: int = 0, part: int = 0) -> dict:
    arg_keys = jax.random.split(jax.random.key(seed), 2)
    part_keys = jax.random.split(jax.random.fold_in(arg_keys[1], part), 2)
    return {
        "features": centred(part_keys[0], (FRAMES, H, W, C), 1.0, 6.0, ((0, 2), (1, 4))),
    }


def halved(current):
    count, height, breadth = current.shape
    return current.reshape(count, height // 2, 2, breadth // 2, 2).mean(axis=(2, 4))

def pyramid_of(frame_now, target):
    own_pixels = frame_now.reshape(H * W, C)
    target_pixels = target.reshape(H * W, C)
    scores = jnp.dot(own_pixels, target_pixels.T, preferred_element_type=jnp.float32) * (1.0 / math.sqrt(C))
    current = scores.reshape(H * W, H, W)
    result = []
    for depth_index in range(4):
        result.append(current.reshape(H, W, -1).astype(jnp.bfloat16))
        if depth_index < 3:
            current = halved(current)
    return tuple(result)

def pair_pyramid(paired):
    return pyramid_of(paired[0], paired[1])

def reference(features):
    blank = jnp.zeros((1, H, W, C), features.dtype)
    following = jnp.concatenate([features[1:], blank], axis=0)
    preceding = jnp.concatenate([blank, features[:-1]], axis=0)
    forward = lax.map(pair_pyramid, (features, following))
    backward = lax.map(pair_pyramid, (features, preceding))
    return (forward[0], forward[1], forward[2], forward[3], backward[0], backward[1], backward[2], backward[3])
```

```python
import functools
import math

import jax
import jax.numpy as jnp
from jax import lax
from jax.experimental import pallas as pl
from jax.experimental.pallas import tpu as pltpu
from jax.sharding import PartitionSpec as P

LEVELS = 4
LANES = 128


def from_behind(value, axis, steps):
    count = lax.axis_size(axis)
    leading, last = (max(0, -steps), min(count, count - steps))
    return lax.ppermute(value, axis, [(source, source + steps) for source in range(leading, last)])


def halved(current):
    count, height, breadth = current.shape
    return current.reshape(count, height // 2, 2, breadth // 2, 2).mean(axis=(2, 4))


def pyramid_of(scores, row_count, breadth):
    height = scores.shape[1] // breadth
    current = scores.reshape(scores.shape[0], height, breadth)
    result = []
    for depth_index in range(LEVELS):
        result.append(current.reshape(1, row_count, breadth, -1).astype(jnp.bfloat16))
        if depth_index < LEVELS - 1:
            current = halved(current)
    return result


def many_frames(features):
    row_count, breadth, channels = features.shape[1:]
    own_pixels = features.reshape(row_count * breadth, channels)
    factor = 1.0 / math.sqrt(channels)
    result = []
    for steps in (-1, 1):
        neighbour = from_behind(own_pixels, "frame", steps)
        target = lax.all_gather(neighbour, "pix", axis=0, tiled=True)
        product = lax.dot_general(
            own_pixels, target, (((1,), (1,)), ((), ())), preferred_element_type=jnp.float32
        )
        result += pyramid_of(product * factor, row_count, breadth)
    return tuple(result)


def dot_nt(left, right):
    return lax.dot_general(left, right, (((1,), (1,)), ((), ())), preferred_element_type=jnp.float32)


def pair_kernel(pix_count, rows, breadth, channels, *refs):
    own_ref, shards = refs[0], refs[1 : 1 + pix_count]
    outs = refs[1 + pix_count : 1 + pix_count + 2 * LEVELS]
    target, summed, pool1, pool2, *values, sems = refs[1 + pix_count + 2 * LEVELS :]
    values, blanks = values[:LEVELS], values[LEVELS:]
    v0, v1, v2, v3 = values
    forward, backward = outs[:LEVELS], outs[LEVELS:]
    frame, pix = lax.axis_index("frame"), lax.axis_index("pix")
    shard = rows * breadth
    height = rows * pix_count
    factor = 1.0 / math.sqrt(channels)

    for blank in blanks:
        blank[...] = jnp.zeros_like(blank)
    for level in range(LEVELS):
        @pl.when(frame == 0)
        def _(level=level):
            pltpu.make_async_copy(blanks[level], backward[level], sems.at[LEVELS + level]).start()

        @pl.when(frame != 0)
        def _(level=level):
            pltpu.make_async_copy(blanks[level], forward[level], sems.at[LEVELS + level]).start()

    def send(level):
        @pl.when(frame == 0)
        def _():
            pltpu.make_async_copy(values[level], forward[level], sems.at[level]).start()

        @pl.when(frame != 0)
        def _():
            pltpu.make_async_copy(values[level], backward[level], sems.at[level]).start()

    for k in range(pix_count):
        at = pl.multiple_of((pix ^ k) * shard, shard)
        target[pl.ds(at, shard), :] = shards[k][...]

    for r in range(rows):
        scores = dot_nt(own_ref[r * breadth : (r + 1) * breadth, :], target[...]) * factor
        v0[r] = scores.astype(v0.dtype)
    send(0)

    def pooled(load, height, breadth):
        half = breadth // 2
        lines = []
        for i in range(height // 2):
            line = load(2 * i) + load(2 * i + 1)
            for c in range(channels // LANES):
                summed[c, i * breadth : (i + 1) * breadth, :] = line[:, c * LANES : (c + 1) * LANES]
        for i in range(height // 2):
            parts = []
            for c in range(channels // LANES):
                even = summed[c, pl.ds(i * breadth, half, stride=2), :]
                odd = summed[c, pl.ds(i * breadth + 1, half, stride=2), :]
                parts.append((even + odd) * 0.25)
            lines.append(jnp.concatenate(parts, axis=1))
        return jnp.concatenate(lines, axis=0)

    def split(value):
        high = value.astype(jnp.bfloat16)
        return high, (value - high.astype(jnp.float32)).astype(jnp.bfloat16)

    level1 = pooled(lambda i: target[i * breadth : (i + 1) * breadth, :].astype(jnp.float32), height, breadth)
    pool1[...] = level1
    b1 = breadth // 2
    level2 = pooled(lambda i: pool1[i * b1 : (i + 1) * b1, :], height // 2, b1)
    pool2[...] = level2
    b2 = breadth // 4
    level3 = pooled(lambda i: pool2[i * b2 : (i + 1) * b2, :], height // 4, b2)

    high, low = split(level1)
    for r in range(rows):
        own = own_ref[r * breadth : (r + 1) * breadth, :]
        v1[r] = ((dot_nt(own, high) + dot_nt(own, low)) * factor).astype(v1.dtype)
    send(1)
    high, low = split(level2)
    for r in range(rows):
        own = own_ref[r * breadth : (r + 1) * breadth, :]
        v2[r] = ((dot_nt(high, own) + dot_nt(low, own)) * factor).astype(v2.dtype)
    send(2)
    high, low = split(level3)
    lines = []
    for r in range(rows):
        own = own_ref[r * breadth : (r + 1) * breadth, :]
        lines.append((dot_nt(high, own) + dot_nt(low, own)) * factor)
    v3[...] = jnp.stack(lines, axis=1).astype(v3.dtype)
    send(3)
    for level in range(LEVELS):
        pltpu.make_async_copy(values[level], forward[level], sems.at[level]).wait()
        pltpu.make_async_copy(blanks[level], backward[level], sems.at[LEVELS + level]).wait()


def two_frames(features):
    rows, breadth, channels = features.shape[1:]
    pix_count = lax.axis_size("pix")
    shard = rows * breadth
    pixels = shard * pix_count
    own = features.reshape(shard, channels)
    shards = []
    for k in reversed(range(pix_count)):
        pairs = [(f * pix_count + p, (1 - f) * pix_count + (p ^ k)) for f in range(2) for p in range(pix_count)]
        shards.append(lax.ppermute(own, ("frame", "pix"), pairs))
    shards = shards[::-1]

    shapes = [
        (rows, breadth, pixels),
        (rows, breadth, pixels // 4),
        (rows, pixels // 16, breadth),
        (pixels // 64, rows, breadth),
    ]
    vmem = pl.BlockSpec(memory_space=pltpu.VMEM)
    outs = pl.pallas_call(
        functools.partial(pair_kernel, pix_count, rows, breadth, channels),
        out_shape=[jax.ShapeDtypeStruct(s, jnp.bfloat16) for s in shapes * 2],
        in_specs=[vmem] * (1 + pix_count),
        out_specs=[pl.BlockSpec(memory_space=pl.ANY)] * (2 * LEVELS),
        scratch_shapes=[
            pltpu.VMEM((pixels, channels), jnp.bfloat16),
            pltpu.VMEM((channels // LANES, pixels // 2, LANES), jnp.float32),
            pltpu.VMEM((pixels // 4, channels), jnp.float32),
            pltpu.VMEM((pixels // 16, channels), jnp.float32),
        ]
        + [pltpu.VMEM(s, jnp.bfloat16) for s in shapes * 2]
        + [pltpu.SemaphoreType.DMA((2 * LEVELS,))],
        cost_estimate=pl.CostEstimate(flops=4 * shard * pixels * channels, bytes_accessed=4 * shard * pixels, transcendentals=0),
    )(own, *shards)
    result = []
    for d in range(2):
        full, half, quarter, eighth = outs[d * LEVELS : (d + 1) * LEVELS]
        result += [full[None], half[None], jnp.transpose(quarter, (0, 2, 1))[None], jnp.transpose(eighth, (1, 2, 0))[None]]
    return tuple(result)


def per_device(frame_count, pix_count, features):
    rows, breadth, channels = features.shape[1:]
    fits = frame_count == 2 and pix_count & (pix_count - 1) == 0 and (rows * pix_count) % 8 == 0 and breadth % 32 == 0 and channels % LANES == 0
    return two_frames(features) if fits else many_frames(features)


def solution(mesh):
    spec = P(("clip", "frame"), "pix", None, None)
    return jax.shard_map(
        functools.partial(per_device, mesh.shape["frame"], mesh.shape["pix"]),
        mesh=mesh,
        in_specs=(spec,),
        out_specs=(spec,) * (2 * LEVELS),
        check_vma=False,
    )
```

```python
import functools
import math

import jax
import jax.numpy as jnp
from jax import lax
from jax.experimental import pallas as pl
from jax.experimental.pallas import tpu as pltpu
from jax.sharding import PartitionSpec as P


LEVELS = 4
LANES = 128


def from_behind(value, axis, steps):
    count = lax.axis_size(axis)
    leading, last = (max(0, -steps), min(count, count - steps))
    return lax.ppermute(value, axis, [(source, source + steps) for source in range(leading, last)])


def halved(current):
    count, height, breadth = current.shape
    return current.reshape(count, height // 2, 2, breadth // 2, 2).mean(axis=(2, 4))


def pyramid_of(scores, row_count, breadth):
    height = scores.shape[1] // breadth
    current = scores.reshape(scores.shape[0], height, breadth)
    result = []
    for depth_index in range(LEVELS):
        result.append(current.reshape(1, row_count, breadth, -1).astype(jnp.bfloat16))
        if depth_index < LEVELS - 1:
            current = halved(current)
    return result


def many_frames(features):
    row_count, breadth, channels = features.shape[1:]
    own_pixels = features.reshape(row_count * breadth, channels)
    factor = 1.0 / math.sqrt(channels)
    result = []
    for steps in (-1, 1):
        neighbour = from_behind(own_pixels, "frame", steps)
        target = lax.all_gather(neighbour, "pix", axis=0, tiled=True)
        product = lax.dot_general(
            own_pixels, target, (((1,), (1,)), ((), ())), preferred_element_type=jnp.float32
        )
        result += pyramid_of(product * factor, row_count, breadth)
    return tuple(result)


def dot_nt(left, right):
    return lax.dot_general(left, right, (((1,), (1,)), ((), ())), preferred_element_type=jnp.float32)


def by_frame(first, second):
    frame = lax.axis_index("frame")
    pl.when(frame == 0)(first)
    pl.when(frame != 0)(second)


def copy_of(source, target, sems, level):
    return pltpu.make_async_copy(source, target, sems.at[level])


def blank_kernel(features_ref, own_ref, *refs):
    outs, (*blanks, sems, own_sem) = refs[: 2 * LEVELS], refs[2 * LEVELS :]
    forward, backward = outs[:LEVELS], outs[LEVELS:]
    fetch = pltpu.make_async_copy(features_ref, own_ref, own_sem)
    fetch.start()
    for blank in blanks:
        blank[...] = jnp.zeros_like(blank)

    def fill(targets):
        def start():
            for level in range(LEVELS):
                copy_of(blanks[level], targets[level], sems, level).start()

        return start

    by_frame(fill(backward), fill(forward))
    for level in range(LEVELS):
        copy_of(blanks[level], backward[level], sems, level).wait()
    fetch.wait()


def pair_kernel(pix_count, rows, breadth, channels, own_ref, *refs):
    origins = origins_of(pix_count)
    shards, refs = refs[: len(origins)], refs[len(origins) + 2 * LEVELS :]
    outs, (target, summed, pool1, pool2, *values, sems) = refs[: 2 * LEVELS], refs[2 * LEVELS :]
    forward, backward = outs[:LEVELS], outs[LEVELS:]
    v0, v1, v2, v3 = values
    pix = lax.axis_index("pix")
    shard = rows * breadth
    height = rows * pix_count
    factor = 1.0 / math.sqrt(channels)

    def send(level):
        def start(targets):
            return lambda: copy_of(values[level], targets[level], sems, level).start()

        by_frame(start(forward), start(backward))

    for ref, origin in zip(shards, origins):
        place = sum(jnp.where(pix == q, p, 0) for q, p in enumerate(origin))
        target[pl.ds(pl.multiple_of(place * shard, shard), shard), :] = ref[...]

    for r in range(rows):
        scores = dot_nt(own_ref[r * breadth : (r + 1) * breadth, :], target[...]) * factor
        v0[r] = scores.astype(v0.dtype)
    send(0)

    def pooled(load, height, breadth):
        half = breadth // 2
        lines = []
        for i in range(height // 2):
            line = load(2 * i) + load(2 * i + 1)
            for c in range(channels // LANES):
                summed[c, i * breadth : (i + 1) * breadth, :] = line[:, c * LANES : (c + 1) * LANES]
        for i in range(height // 2):
            parts = []
            for c in range(channels // LANES):
                even = summed[c, pl.ds(i * breadth, half, stride=2), :]
                odd = summed[c, pl.ds(i * breadth + 1, half, stride=2), :]
                parts.append((even + odd) * 0.25)
            lines.append(jnp.concatenate(parts, axis=1))
        return jnp.concatenate(lines, axis=0)

    def split(value):
        high = value.astype(jnp.bfloat16)
        return high, (value - high.astype(jnp.float32)).astype(jnp.bfloat16)

    level1 = pooled(lambda i: target[i * breadth : (i + 1) * breadth, :].astype(jnp.float32), height, breadth)
    pool1[...] = level1
    b1 = breadth // 2
    level2 = pooled(lambda i: pool1[i * b1 : (i + 1) * b1, :], height // 2, b1)
    pool2[...] = level2
    b2 = breadth // 4
    level3 = pooled(lambda i: pool2[i * b2 : (i + 1) * b2, :], height // 4, b2)

    high, low = split(level1)
    for r in range(rows):
        own = own_ref[r * breadth : (r + 1) * breadth, :]
        v1[r] = ((dot_nt(own, high) + dot_nt(own, low)) * factor).astype(v1.dtype)
    send(1)
    high, low = split(level2)
    for r in range(rows):
        own = own_ref[r * breadth : (r + 1) * breadth, :]
        v2[r] = ((dot_nt(high, own) + dot_nt(low, own)) * factor).astype(v2.dtype)
    send(2)
    high, low = split(level3)
    lines = []
    for r in range(rows):
        own = own_ref[r * breadth : (r + 1) * breadth, :]
        lines.append((dot_nt(high, own) + dot_nt(low, own)) * factor)
    v3[...] = jnp.stack(lines, axis=1).astype(v3.dtype)
    send(3)
    for level in range(LEVELS):
        copy_of(values[level], forward[level], sems, level).wait()


def rounds_of(pix_count):
    if pix_count == 4:
        return [[2, 0, 3, 1], [1, 3, 0, 2], [0, 2, 1, 3]], True
    return [[p ^ k for p in range(pix_count)] for k in range(pix_count)], False


def origins_of(pix_count):
    rounds, relayed = rounds_of(pix_count)
    origins = [[row.index(q) for q in range(pix_count)] for row in rounds]
    return origins + ([[rounds[0].index(q ^ 1) for q in range(pix_count)]] if relayed else [])


def exchange(own, pix_count):
    rounds, relayed = rounds_of(pix_count)
    got = []
    for row in rounds:
        pairs = [(f * pix_count + p, (1 - f) * pix_count + row[p]) for f in range(2) for p in range(pix_count)]
        got.append(lax.ppermute(own, ("frame", "pix"), pairs))
    if relayed:
        got.append(lax.ppermute(got[0], "pix", [(p, p ^ 1) for p in range(pix_count)]))
    return got


def two_frames(features):
    rows, breadth, channels = features.shape[1:]
    pix_count = lax.axis_size("pix")
    shard = rows * breadth
    pixels = shard * pix_count
    own = features.reshape(shard, channels)
    shards = exchange(own, pix_count)
    count = len(shards)

    shapes = [
        (rows, breadth, pixels),
        (rows, breadth, pixels // 4),
        (rows, pixels // 16, breadth),
        (pixels // 64, rows, breadth),
    ]
    vmem = pl.BlockSpec(memory_space=pltpu.VMEM)
    anywhere = pl.BlockSpec(memory_space=pl.ANY)
    out_shapes = [jax.ShapeDtypeStruct(s, jnp.bfloat16) for s in shapes * 2]
    staging = [pltpu.VMEM(s, jnp.bfloat16) for s in shapes]
    limits = pltpu.CompilerParams(vmem_limit_bytes=16 * 2**20)
    near, *blanks = pl.pallas_call(
        blank_kernel,
        out_shape=[jax.ShapeDtypeStruct(own.shape, own.dtype)] + out_shapes,
        in_specs=[anywhere],
        out_specs=[vmem] + [anywhere] * (2 * LEVELS),
        scratch_shapes=staging + [pltpu.SemaphoreType.DMA((LEVELS,)), pltpu.SemaphoreType.DMA],
        compiler_params=limits,
        cost_estimate=pl.CostEstimate(flops=shard * pixels * channels, bytes_accessed=4 * shard * pixels, transcendentals=0),
    )(own)
    outs = pl.pallas_call(
        functools.partial(pair_kernel, pix_count, rows, breadth, channels),
        out_shape=out_shapes,
        in_specs=[vmem] * (1 + count) + [anywhere] * (2 * LEVELS),
        out_specs=[anywhere] * (2 * LEVELS),
        scratch_shapes=[
            pltpu.VMEM((pixels, channels), jnp.bfloat16),
            pltpu.VMEM((channels // LANES, pixels // 2, LANES), jnp.float32),
            pltpu.VMEM((pixels // 4, channels), jnp.float32),
            pltpu.VMEM((pixels // 16, channels), jnp.float32),
        ]
        + staging
        + [pltpu.SemaphoreType.DMA((LEVELS,))],
        input_output_aliases={1 + count + i: i for i in range(2 * LEVELS)},
        compiler_params=limits,
        cost_estimate=pl.CostEstimate(flops=4 * shard * pixels * channels, bytes_accessed=4 * shard * pixels, transcendentals=0),
    )(near, *shards, *blanks)
    result = []
    for d in range(2):
        full, half, quarter, eighth = outs[d * LEVELS : (d + 1) * LEVELS]
        result += [full[None], half[None], jnp.transpose(quarter, (0, 2, 1))[None], jnp.transpose(eighth, (1, 2, 0))[None]]
    return tuple(result)


def per_device(frame_count, pix_count, features):
    rows, breadth, channels = features.shape[1:]
    fits = frame_count == 2 and pix_count & (pix_count - 1) == 0 and (rows * pix_count) % 8 == 0 and breadth % 32 == 0 and channels % LANES == 0
    return two_frames(features) if fits else many_frames(features)


def solution(mesh):
    spec = P(("clip", "frame"), "pix", None, None)

    def body(features):
        return per_device(mesh.shape["frame"], mesh.shape["pix"], features)

    return jax.shard_map(
        body, mesh=mesh, in_specs=(spec,), out_specs=(spec,) * (2 * LEVELS), check_vma=False
    )
```

```python
import functools
import math

import jax
import jax.numpy as jnp
from jax import lax
from jax.experimental import pallas as pl
from jax.experimental.pallas import tpu as pltpu
from jax.sharding import PartitionSpec as P


LEVELS = 4
LANES = 128


def from_behind(value, axis, steps):
    count = lax.axis_size(axis)
    leading, last = (max(0, -steps), min(count, count - steps))
    return lax.ppermute(value, axis, [(source, source + steps) for source in range(leading, last)])


def halved(current):
    count, height, breadth = current.shape
    return current.reshape(count, height // 2, 2, breadth // 2, 2).mean(axis=(2, 4))


def pyramid_of(scores, row_count, breadth):
    height = scores.shape[1] // breadth
    current = scores.reshape(scores.shape[0], height, breadth)
    result = []
    for depth_index in range(LEVELS):
        result.append(current.reshape(1, row_count, breadth, -1).astype(jnp.bfloat16))
        if depth_index < LEVELS - 1:
            current = halved(current)
    return result


def many_frames(features):
    row_count, breadth, channels = features.shape[1:]
    own_pixels = features.reshape(row_count * breadth, channels)
    factor = 1.0 / math.sqrt(channels)
    result = []
    for steps in (-1, 1):
        neighbour = from_behind(own_pixels, "frame", steps)
        target = lax.all_gather(neighbour, "pix", axis=0, tiled=True)
        product = lax.dot_general(
            own_pixels, target, (((1,), (1,)), ((), ())), preferred_element_type=jnp.float32
        )
        result += pyramid_of(product * factor, row_count, breadth)
    return tuple(result)


def dot_nt(left, right):
    return lax.dot_general(left, right, (((1,), (1,)), ((), ())), preferred_element_type=jnp.float32)


def by_frame(first, second):
    frame = lax.axis_index("frame")
    pl.when(frame == 0)(first)
    pl.when(frame != 0)(second)


def send(level, piece, source, forward, backward, sems, columns=None):
    def start(targets):
        target = targets[level] if columns is None else targets[level].at[:, :, columns]
        return lambda: pltpu.make_async_copy(source, target, sems.at[piece]).start()

    by_frame(start(forward), start(backward))


def blank_kernel(features_ref, own_ref, *refs):
    outs, (*blanks, sems, own_sem) = refs[: 2 * LEVELS], refs[2 * LEVELS :]
    forward, backward = outs[:LEVELS], outs[LEVELS:]
    fetch = pltpu.make_async_copy(features_ref, own_ref, own_sem)
    fetch.start()
    for level, blank in enumerate(blanks):
        blank[...] = jnp.zeros_like(blank)
        send(level, level, blank, backward, forward, sems)
    for level, blank in enumerate(blanks):
        pltpu.make_async_copy(blank, backward[level], sems.at[level]).wait()
    fetch.wait()


def place_of(origin):
    pix = lax.axis_index("pix")
    return sum(jnp.where(pix == q, p, 0) for q, p in enumerate(origin))


def paired(line, summed, breadth):
    parts = []
    for c in range(line.shape[1] // LANES):
        summed[c, :breadth, :] = line[:, c * LANES : (c + 1) * LANES]
    for c in range(line.shape[1] // LANES):
        even = summed[c, pl.ds(0, breadth // 2, stride=2), :]
        odd = summed[c, pl.ds(1, breadth // 2, stride=2), :]
        parts.append((even + odd) * 0.25)
    return jnp.concatenate(parts, axis=1)


def level1_of(shard_ref, summed, breadth):
    upper = shard_ref[:breadth, :].astype(jnp.float32)
    return paired(upper + shard_ref[breadth : 2 * breadth, :].astype(jnp.float32), summed, breadth)


def split(value):
    high = value.astype(jnp.bfloat16)
    return high, (value - high.astype(jnp.float32)).astype(jnp.bfloat16)


def early_kernel(pix_count, breadth, own_ref, *refs):
    origins = origins_of(pix_count)
    count = len(origins) - 1
    shards, (scores_ref, partner_ref, high_ref, low_ref, partner1_ref, level2_ref) = refs[:count], refs[count : count + 6]
    target, level1, *summed = refs[count + 6 :]
    shard = own_ref.shape[0]
    half = breadth // 2
    last = place_of(origins[-1])
    far = 1 - last // 2
    factor = 1.0 / math.sqrt(own_ref.shape[1])
    for i, ref in enumerate(shards):
        place = place_of(origins[i])
        target[pl.ds(pl.multiple_of(place * shard, shard), shard), :] = ref[...]
        means = level1_of(ref, summed[i], breadth)
        at = pl.ds(pl.multiple_of(place * half, half), half)
        level1[at, :] = means
        high_ref[at, :], low_ref[at, :] = split(means)
    pair = target[pl.ds(pl.multiple_of(far * 2 * shard, 2 * shard), 2 * shard), :]
    scores = (dot_nt(own_ref[...], pair) * factor).astype(scores_ref.dtype)
    for r in range(2):
        scores_ref[r] = scores[r * breadth : (r + 1) * breadth, :]
    partner = last + 1 - 2 * (last % 2)
    partner_ref[...] = target[pl.ds(pl.multiple_of(partner * shard, shard), shard), :]
    partner1_ref[...] = level1[pl.ds(pl.multiple_of(partner * half, half), half), :]
    upper = level1[pl.ds(pl.multiple_of(far * breadth, half), half), :]
    lower = level1[pl.ds(pl.multiple_of(far * breadth + half, half), half), :]
    level2_ref[...] = paired(upper + lower, summed[0], half)


def late_kernel(pix_count, breadth, *refs):
    own_ref, relayed_ref, scores_ref, partner_ref, high_ref, low_ref, partner1_ref, far2_ref = refs[:8]
    outs, (target, highs, lows, level2, level3, summed, near_scores, v1, v2, v3, sems) = refs[8 + 2 * LEVELS : 8 + 4 * LEVELS], refs[8 + 4 * LEVELS :]
    forward, backward = outs[:LEVELS], outs[LEVELS:]
    shard = own_ref.shape[0]
    half, quarter = breadth // 2, breadth // 4
    last = place_of(origins_of(pix_count)[-1])
    near = last // 2
    far = 1 - near
    factor = 1.0 / math.sqrt(own_ref.shape[1])

    def columns(pair):
        return pl.ds(pl.multiple_of(pair * 2 * shard, 2 * shard), 2 * shard)

    send(0, LEVELS, scores_ref, forward, backward, sems, columns(far))
    odd = last % 2
    target[pl.ds(pl.multiple_of(odd * shard, shard), shard), :] = relayed_ref[...]
    target[pl.ds(pl.multiple_of((1 - odd) * shard, shard), shard), :] = partner_ref[...]
    level1 = level1_of(relayed_ref, summed, breadth)
    highs[...] = high_ref[...]
    lows[...] = low_ref[...]
    at = pl.ds(pl.multiple_of(last * half, half), half)
    highs[at, :], lows[at, :] = split(level1)
    level2[pl.ds(pl.multiple_of(near * quarter, quarter), quarter), :] = paired(level1 + partner1_ref[...], summed, half)
    level2[pl.ds(pl.multiple_of(far * quarter, quarter), quarter), :] = far2_ref[...]
    eighth = quarter // 2
    level3[...] = jnp.zeros_like(level3)
    level3[:eighth, :] = paired(level2[:quarter, :] + level2[quarter:, :], summed, quarter)
    own = own_ref[...]
    scores = (dot_nt(own, target[...]) * factor).astype(near_scores.dtype)
    halves = ((dot_nt(own, highs[...]) + dot_nt(own, lows[...])) * factor).astype(v1.dtype)
    coarse = jnp.concatenate([*split(level2[...]), *split(level3[...])], axis=0)
    lines = []
    for r in range(2):
        near_scores[r] = scores[r * breadth : (r + 1) * breadth, :]
        v1[r] = halves[r * breadth : (r + 1) * breadth, :]
        product = dot_nt(coarse, own[r * breadth : (r + 1) * breadth, :]) * factor
        v2[r] = (product[:half, :] + product[half:breadth, :]).astype(v2.dtype)
        product = product[breadth:, :]
        lines.append(product[:eighth, :] + product[level3.shape[0] : level3.shape[0] + eighth, :])
    v3[...] = jnp.stack(lines, axis=1).astype(v3.dtype)
    pieces = ((0, 0, near_scores, columns(near)), (1, 1, v1, None), (2, 2, v2, None), (3, 3, v3, None))

    def start(targets):
        def run():
            for level, piece, source, where in pieces:
                target = targets[level] if where is None else targets[level].at[:, :, where]
                pltpu.make_async_copy(source, target, sems.at[piece]).start()

        return run

    by_frame(start(forward), start(backward))
    pltpu.make_async_copy(scores_ref, forward[0].at[:, :, columns(far)], sems.at[LEVELS]).wait()
    pltpu.make_async_copy(near_scores, forward[0].at[:, :, columns(near)], sems.at[0]).wait()
    for level, value in ((1, v1), (2, v2), (3, v3)):
        pltpu.make_async_copy(value, forward[level], sems.at[level]).wait()


ROUNDS = ((2, 0, 3, 1), (1, 3, 0, 2), (0, 2, 1, 3))


def origins_of(pix_count):
    origins = [[row.index(q) for q in range(pix_count)] for row in ROUNDS]
    return origins + [[ROUNDS[0].index(q ^ 1) for q in range(pix_count)]]


def exchange(own, pix_count):
    got = []
    for row in ROUNDS:
        pairs = [(f * pix_count + p, (1 - f) * pix_count + row[p]) for f in range(2) for p in range(pix_count)]
        got.append(lax.ppermute(own, ("frame", "pix"), pairs))
    got.append(lax.ppermute(got[0], "pix", [(p, p ^ 1) for p in range(pix_count)]))
    return got


def two_frames(features):
    rows, breadth, channels = features.shape[1:]
    pix_count = lax.axis_size("pix")
    shard = rows * breadth
    pixels = shard * pix_count
    own = features.reshape(shard, channels)
    *direct, relayed = exchange(own, pix_count)

    shapes = [
        (rows, breadth, pixels),
        (rows, breadth, pixels // 4),
        (rows, pixels // 16, breadth),
        (pixels // 64, rows, breadth),
    ]
    vmem = pl.BlockSpec(memory_space=pltpu.VMEM)
    anywhere = pl.BlockSpec(memory_space=pl.ANY)
    hbm = pl.BlockSpec(memory_space=pltpu.HBM)
    out_shapes = [jax.ShapeDtypeStruct(s, jnp.bfloat16) for s in shapes * 2]
    limits = pltpu.CompilerParams(vmem_limit_bytes=12 * 2**20)

    def cost(flops):
        return pl.CostEstimate(flops=flops, bytes_accessed=4 * shard * pixels, transcendentals=0)

    def scratch(kind, *shape):
        return pltpu.VMEM(shape, kind)

    flops = shard * pixels * channels
    near, *blanks = pl.pallas_call(
        blank_kernel,
        out_shape=[jax.ShapeDtypeStruct(own.shape, own.dtype)] + out_shapes,
        in_specs=[hbm],
        out_specs=[vmem] + [anywhere] * (2 * LEVELS),
        scratch_shapes=[scratch(jnp.bfloat16, *s) for s in shapes]
        + [pltpu.SemaphoreType.DMA((LEVELS,)), pltpu.SemaphoreType.DMA],
        compiler_params=limits,
        cost_estimate=cost(flops),
    )(own)
    early = pl.pallas_call(
        functools.partial(early_kernel, pix_count, breadth),
        out_shape=[
            jax.ShapeDtypeStruct((rows, breadth, 2 * shard), jnp.bfloat16),
            jax.ShapeDtypeStruct((shard, channels), jnp.bfloat16),
            jax.ShapeDtypeStruct((pixels // 4, channels), jnp.bfloat16),
            jax.ShapeDtypeStruct((pixels // 4, channels), jnp.bfloat16),
            jax.ShapeDtypeStruct((shard // 4, channels), jnp.float32),
            jax.ShapeDtypeStruct((shard // 8, channels), jnp.float32),
        ],
        in_specs=[vmem] * (1 + len(direct)),
        out_specs=[vmem] * 6,
        scratch_shapes=[
            scratch(jnp.bfloat16, pixels, channels),
            scratch(jnp.float32, pixels // 4, channels),
        ]
        + [scratch(jnp.float32, channels // LANES, breadth, LANES)] * len(direct),
        compiler_params=limits,
        cost_estimate=cost(2 * flops),
    )(near, *direct)
    outs = pl.pallas_call(
        functools.partial(late_kernel, pix_count, breadth),
        out_shape=out_shapes,
        in_specs=[vmem] * 8 + [anywhere] * (2 * LEVELS),
        out_specs=[anywhere] * (2 * LEVELS),
        scratch_shapes=[
            scratch(jnp.bfloat16, 2 * shard, channels),
            scratch(jnp.bfloat16, pixels // 4, channels),
            scratch(jnp.bfloat16, pixels // 4, channels),
            scratch(jnp.float32, pixels // 16, channels),
            scratch(jnp.float32, -(-pixels // 64 // 16) * 16, channels),
            scratch(jnp.float32, channels // LANES, breadth, LANES),
            scratch(jnp.bfloat16, rows, breadth, 2 * shard),
        ]
        + [scratch(jnp.bfloat16, *s) for s in shapes[1:]]
        + [pltpu.SemaphoreType.DMA((LEVELS + 1,))],
        input_output_aliases={8 + i: i for i in range(2 * LEVELS)},
        compiler_params=limits,
        cost_estimate=cost(2 * flops),
    )(near, relayed, *early, *blanks)
    result = []
    for d in range(2):
        full, half, quarter, eighth = outs[d * LEVELS : (d + 1) * LEVELS]
        result += [full[None], half[None], jnp.transpose(quarter, (0, 2, 1))[None], jnp.transpose(eighth, (1, 2, 0))[None]]
    return tuple(result)


def per_device(frame_count, pix_count, features):
    rows, breadth, channels = features.shape[1:]
    fits = frame_count == 2 and pix_count == len(ROUNDS) + 1 and rows == 2 and breadth % 32 == 0 and channels % LANES == 0
    return two_frames(features) if fits and 2 * rows * breadth % LANES == 0 else many_frames(features)


def solution(mesh):
    spec = P(("clip", "frame"), "pix", None, None)

    def body(features):
        return per_device(mesh.shape["frame"], mesh.shape["pix"], features)

    return jax.shard_map(
        body, mesh=mesh, in_specs=(spec,), out_specs=(spec,) * (2 * LEVELS), check_vma=False
    )
```

```python
import functools
import math

import jax
import jax.numpy as jnp
from jax import lax
from jax.experimental import pallas as pl
from jax.experimental.pallas import tpu as pltpu
from jax.sharding import PartitionSpec as P


LEVELS = 4
LANES = 128


def from_behind(value, axis, steps):
    count = lax.axis_size(axis)
    leading, last = (max(0, -steps), min(count, count - steps))
    return lax.ppermute(value, axis, [(source, source + steps) for source in range(leading, last)])


def halved(current):
    count, height, breadth = current.shape
    return current.reshape(count, height // 2, 2, breadth // 2, 2).mean(axis=(2, 4))


def pyramid_of(scores, row_count, breadth):
    height = scores.shape[1] // breadth
    current = scores.reshape(scores.shape[0], height, breadth)
    result = []
    for depth_index in range(LEVELS):
        result.append(current.reshape(1, row_count, breadth, -1).astype(jnp.bfloat16))
        if depth_index < LEVELS - 1:
            current = halved(current)
    return result


def many_frames(features):
    row_count, breadth, channels = features.shape[1:]
    own_pixels = features.reshape(row_count * breadth, channels)
    factor = 1.0 / math.sqrt(channels)
    result = []
    for steps in (-1, 1):
        neighbour = from_behind(own_pixels, "frame", steps)
        target = lax.all_gather(neighbour, "pix", axis=0, tiled=True)
        product = lax.dot_general(
            own_pixels, target, (((1,), (1,)), ((), ())), preferred_element_type=jnp.float32
        )
        result += pyramid_of(product * factor, row_count, breadth)
    return tuple(result)


def dot_nt(left, right):
    return lax.dot_general(left, right, (((1,), (1,)), ((), ())), preferred_element_type=jnp.float32)


def by_frame(first, second):
    frame = lax.axis_index("frame")
    pl.when(frame == 0)(first)
    pl.when(frame != 0)(second)


def send(level, piece, source, forward, backward, sems, columns=None):
    def start(targets):
        target = targets[level] if columns is None else targets[level].at[:, :, columns]
        return lambda: pltpu.make_async_copy(source, target, sems.at[piece]).start()

    by_frame(start(forward), start(backward))


def blank_kernel(features_ref, own_ref, *refs):
    outs, (*blanks, sems, own_sem) = refs[: 2 * LEVELS], refs[2 * LEVELS :]
    forward, backward = outs[:LEVELS], outs[LEVELS:]
    fetch = pltpu.make_async_copy(features_ref, own_ref, own_sem)
    fetch.start()
    for level, blank in enumerate(blanks):
        blank[...] = jnp.zeros_like(blank)
        send(level, level, blank, backward, forward, sems)
    for level, blank in enumerate(blanks):
        pltpu.make_async_copy(blank, backward[level], sems.at[level]).wait()
    fetch.wait()


def place_of(origin):
    pix = lax.axis_index("pix")
    return sum(jnp.where(pix == q, p, 0) for q, p in enumerate(origin))


def pooled(line, summed, step):
    breadth = line.shape[0]
    parts = []
    for c in range(line.shape[1] // LANES):
        summed[c] = line[:, c * LANES : (c + 1) * LANES]
    for c in range(line.shape[1] // LANES):
        total = summed[c, pl.ds(0, breadth // step, stride=step), :]
        for i in range(1, step):
            total = total + summed[c, pl.ds(i, breadth // step, stride=step), :]
        parts.append(total * (1.0 / (step * step)))
    return jnp.concatenate(parts, axis=1)


def line_of(shard_ref, breadth):
    return shard_ref[:breadth, :].astype(jnp.float32) + shard_ref[breadth : 2 * breadth, :].astype(jnp.float32)


def split(value):
    high = value.astype(jnp.bfloat16)
    return high, (value - high.astype(jnp.float32)).astype(jnp.bfloat16)


def early_kernel(pix_count, breadth, own_ref, *refs):
    origins = origins_of(pix_count)
    count = len(origins) - 1
    shards, (scores_ref, partner_ref, high_ref, low_ref, partner_line_ref, far_line_ref, far2_ref) = refs[:count], refs[count : count + 7]
    target, lines, *summed = refs[count + 7 :]
    shard = own_ref.shape[0]
    half = breadth // 2
    last = place_of(origins[-1])
    far = 1 - last // 2
    factor = 1.0 / math.sqrt(own_ref.shape[1])
    for i, ref in enumerate(shards):
        place = place_of(origins[i])
        target[pl.ds(pl.multiple_of(place * shard, shard), shard), :] = ref[...]
        line = line_of(ref, breadth)
        lines[pl.ds(pl.multiple_of(place * breadth, breadth), breadth), :] = line
        at = pl.ds(pl.multiple_of(place * half, half), half)
        high_ref[at, :], low_ref[at, :] = split(pooled(line, summed[i], 2))
    pair = target[pl.ds(pl.multiple_of(far * 2 * shard, 2 * shard), 2 * shard), :]
    scores = (dot_nt(own_ref[...], pair) * factor).astype(scores_ref.dtype)
    for r in range(2):
        scores_ref[r] = scores[r * breadth : (r + 1) * breadth, :]
    partner = last + 1 - 2 * (last % 2)
    partner_ref[...] = target[pl.ds(pl.multiple_of(partner * shard, shard), shard), :]
    partner_line_ref[...] = lines[pl.ds(pl.multiple_of(partner * breadth, breadth), breadth), :]
    upper = lines[pl.ds(pl.multiple_of(far * 2 * breadth, breadth), breadth), :]
    far_line = upper + lines[pl.ds(pl.multiple_of((far * 2 + 1) * breadth, breadth), breadth), :]
    far_line_ref[...] = far_line
    far2_ref[...] = pooled(far_line, summed[0], 4)


def late_kernel(pix_count, breadth, *refs):
    own_ref, relayed_ref, scores_ref, partner_ref, high_ref, low_ref, partner_line_ref, far_line_ref, far2_ref = refs[:9]
    outs, (target, highs, lows, level2, level3, sum1, sum2, sum3, near_scores, v1, v2, v3, sems) = refs[9 + 2 * LEVELS : 9 + 4 * LEVELS], refs[9 + 4 * LEVELS :]
    forward, backward = outs[:LEVELS], outs[LEVELS:]
    shard = own_ref.shape[0]
    half, quarter = breadth // 2, breadth // 4
    last = place_of(origins_of(pix_count)[-1])
    near = last // 2
    far = 1 - near
    factor = 1.0 / math.sqrt(own_ref.shape[1])

    def columns(pair):
        return pl.ds(pl.multiple_of(pair * 2 * shard, 2 * shard), 2 * shard)

    send(0, LEVELS, scores_ref, forward, backward, sems, columns(far))
    odd = last % 2
    target[pl.ds(pl.multiple_of(odd * shard, shard), shard), :] = relayed_ref[...]
    target[pl.ds(pl.multiple_of((1 - odd) * shard, shard), shard), :] = partner_ref[...]
    line = line_of(relayed_ref, breadth)
    near_line = line + partner_line_ref[...]
    highs[...] = high_ref[...]
    lows[...] = low_ref[...]
    at = pl.ds(pl.multiple_of(last * half, half), half)
    highs[at, :], lows[at, :] = split(pooled(line, sum1, 2))
    level2[pl.ds(pl.multiple_of(near * quarter, quarter), quarter), :] = pooled(near_line, sum2, 4)
    level2[pl.ds(pl.multiple_of(far * quarter, quarter), quarter), :] = far2_ref[...]
    eighth = quarter // 2
    level3[...] = jnp.zeros_like(level3)
    level3[:eighth, :] = pooled(near_line + far_line_ref[...], sum3, 8)
    own = own_ref[...]
    scores = (dot_nt(own, target[...]) * factor).astype(near_scores.dtype)
    halves = ((dot_nt(own, highs[...]) + dot_nt(own, lows[...])) * factor).astype(v1.dtype)
    coarse = jnp.concatenate([*split(level2[...]), *split(level3[...])], axis=0)
    lines = []
    for r in range(2):
        near_scores[r] = scores[r * breadth : (r + 1) * breadth, :]
        v1[r] = halves[r * breadth : (r + 1) * breadth, :]
        product = dot_nt(coarse, own[r * breadth : (r + 1) * breadth, :]) * factor
        v2[r] = (product[:half, :] + product[half:breadth, :]).astype(v2.dtype)
        product = product[breadth:, :]
        lines.append(product[:eighth, :] + product[level3.shape[0] : level3.shape[0] + eighth, :])
    v3[...] = jnp.stack(lines, axis=1).astype(v3.dtype)
    pieces = ((0, 0, near_scores, columns(near)), (1, 1, v1, None), (2, 2, v2, None), (3, 3, v3, None))

    def start(targets):
        def run():
            for level, piece, source, where in pieces:
                target = targets[level] if where is None else targets[level].at[:, :, where]
                pltpu.make_async_copy(source, target, sems.at[piece]).start()

        return run

    by_frame(start(forward), start(backward))
    pltpu.make_async_copy(scores_ref, forward[0].at[:, :, columns(far)], sems.at[LEVELS]).wait()
    pltpu.make_async_copy(near_scores, forward[0].at[:, :, columns(near)], sems.at[0]).wait()
    for level, value in ((1, v1), (2, v2), (3, v3)):
        pltpu.make_async_copy(value, forward[level], sems.at[level]).wait()


ROUNDS = ((2, 0, 3, 1), (1, 3, 0, 2), (0, 2, 1, 3))


def origins_of(pix_count):
    origins = [[row.index(q) for q in range(pix_count)] for row in ROUNDS]
    return origins + [[ROUNDS[0].index(q ^ 1) for q in range(pix_count)]]


def exchange(own, pix_count):
    got = []
    for row in ROUNDS:
        pairs = [(f * pix_count + p, (1 - f) * pix_count + row[p]) for f in range(2) for p in range(pix_count)]
        got.append(lax.ppermute(own, ("frame", "pix"), pairs))
    got.append(lax.ppermute(got[0], "pix", [(p, p ^ 1) for p in range(pix_count)]))
    return got


def two_frames(features):
    rows, breadth, channels = features.shape[1:]
    pix_count = lax.axis_size("pix")
    shard = rows * breadth
    pixels = shard * pix_count
    own = features.reshape(shard, channels)
    *direct, relayed = exchange(own, pix_count)

    shapes = [
        (rows, breadth, pixels),
        (rows, breadth, pixels // 4),
        (rows, pixels // 16, breadth),
        (pixels // 64, rows, breadth),
    ]
    vmem = pl.BlockSpec(memory_space=pltpu.VMEM)
    anywhere = pl.BlockSpec(memory_space=pl.ANY)
    hbm = pl.BlockSpec(memory_space=pltpu.HBM)
    out_shapes = [jax.ShapeDtypeStruct(s, jnp.bfloat16) for s in shapes * 2]
    limits = pltpu.CompilerParams(vmem_limit_bytes=12 * 2**20)

    def cost(flops):
        return pl.CostEstimate(flops=flops, bytes_accessed=4 * shard * pixels, transcendentals=0)

    def scratch(kind, *shape):
        return pltpu.VMEM(shape, kind)

    flops = shard * pixels * channels
    near, *blanks = pl.pallas_call(
        blank_kernel,
        out_shape=[jax.ShapeDtypeStruct(own.shape, own.dtype)] + out_shapes,
        in_specs=[hbm],
        out_specs=[vmem] + [anywhere] * (2 * LEVELS),
        scratch_shapes=[scratch(jnp.bfloat16, *s) for s in shapes]
        + [pltpu.SemaphoreType.DMA((LEVELS,)), pltpu.SemaphoreType.DMA],
        compiler_params=limits,
        cost_estimate=cost(flops),
    )(own)
    early = pl.pallas_call(
        functools.partial(early_kernel, pix_count, breadth),
        out_shape=[
            jax.ShapeDtypeStruct((rows, breadth, 2 * shard), jnp.bfloat16),
            jax.ShapeDtypeStruct((shard, channels), jnp.bfloat16),
            jax.ShapeDtypeStruct((pixels // 4, channels), jnp.bfloat16),
            jax.ShapeDtypeStruct((pixels // 4, channels), jnp.bfloat16),
            jax.ShapeDtypeStruct((breadth, channels), jnp.float32),
            jax.ShapeDtypeStruct((breadth, channels), jnp.float32),
            jax.ShapeDtypeStruct((shard // 8, channels), jnp.float32),
        ],
        in_specs=[vmem] * (1 + len(direct)),
        out_specs=[vmem] * 7,
        scratch_shapes=[
            scratch(jnp.bfloat16, pixels, channels),
            scratch(jnp.float32, pix_count * breadth, channels),
        ]
        + [scratch(jnp.float32, channels // LANES, breadth, LANES)] * len(direct),
        compiler_params=limits,
        cost_estimate=cost(2 * flops),
    )(near, *direct)
    outs = pl.pallas_call(
        functools.partial(late_kernel, pix_count, breadth),
        out_shape=out_shapes,
        in_specs=[vmem] * 9 + [anywhere] * (2 * LEVELS),
        out_specs=[anywhere] * (2 * LEVELS),
        scratch_shapes=[
            scratch(jnp.bfloat16, 2 * shard, channels),
            scratch(jnp.bfloat16, pixels // 4, channels),
            scratch(jnp.bfloat16, pixels // 4, channels),
            scratch(jnp.float32, pixels // 16, channels),
            scratch(jnp.float32, -(-pixels // 64 // 16) * 16, channels),
            scratch(jnp.float32, channels // LANES, breadth, LANES),
            scratch(jnp.float32, channels // LANES, breadth, LANES),
            scratch(jnp.float32, channels // LANES, breadth, LANES),
            scratch(jnp.bfloat16, rows, breadth, 2 * shard),
        ]
        + [scratch(jnp.bfloat16, *s) for s in shapes[1:]]
        + [pltpu.SemaphoreType.DMA((LEVELS + 1,))],
        input_output_aliases={9 + i: i for i in range(2 * LEVELS)},
        compiler_params=limits,
        cost_estimate=cost(2 * flops),
    )(near, relayed, *early, *blanks)
    result = []
    for d in range(2):
        full, half, quarter, eighth = outs[d * LEVELS : (d + 1) * LEVELS]
        result += [full[None], half[None], jnp.transpose(quarter, (0, 2, 1))[None], jnp.transpose(eighth, (1, 2, 0))[None]]
    return tuple(result)


def per_device(frame_count, pix_count, features):
    rows, breadth, channels = features.shape[1:]
    fits = frame_count == 2 and pix_count == len(ROUNDS) + 1 and rows == 2 and breadth % 32 == 0 and channels % LANES == 0
    return two_frames(features) if fits and 2 * rows * breadth % LANES == 0 else many_frames(features)


def solution(mesh):
    spec = P(("clip", "frame"), "pix", None, None)

    def body(features):
        return per_device(mesh.shape["frame"], mesh.shape["pix"], features)

    return jax.shard_map(
        body, mesh=mesh, in_specs=(spec,), out_specs=(spec,) * (2 * LEVELS), check_vma=False
    )
```

```python
import functools
import math

import jax
import jax.numpy as jnp
from jax import lax
from jax.experimental import pallas as pl
from jax.experimental.pallas import tpu as pltpu
from jax.sharding import PartitionSpec as P


LEVELS = 4
LANES = 128


def from_behind(value, axis, steps):
    count = lax.axis_size(axis)
    leading, last = (max(0, -steps), min(count, count - steps))
    return lax.ppermute(value, axis, [(source, source + steps) for source in range(leading, last)])


def halved(current):
    count, height, breadth = current.shape
    return current.reshape(count, height // 2, 2, breadth // 2, 2).mean(axis=(2, 4))


def pyramid_of(scores, row_count, breadth):
    height = scores.shape[1] // breadth
    current = scores.reshape(scores.shape[0], height, breadth)
    result = []
    for depth_index in range(LEVELS):
        result.append(current.reshape(1, row_count, breadth, -1).astype(jnp.bfloat16))
        if depth_index < LEVELS - 1:
            current = halved(current)
    return result


def many_frames(features):
    row_count, breadth, channels = features.shape[1:]
    own_pixels = features.reshape(row_count * breadth, channels)
    factor = 1.0 / math.sqrt(channels)
    result = []
    for steps in (-1, 1):
        neighbour = from_behind(own_pixels, "frame", steps)
        target = lax.all_gather(neighbour, "pix", axis=0, tiled=True)
        product = lax.dot_general(
            own_pixels, target, (((1,), (1,)), ((), ())), preferred_element_type=jnp.float32
        )
        result += pyramid_of(product * factor, row_count, breadth)
    return tuple(result)


def dot_nt(left, right):
    return lax.dot_general(left, right, (((1,), (1,)), ((), ())), preferred_element_type=jnp.float32)


def by_frame(first, second):
    frame = lax.axis_index("frame")
    pl.when(frame == 0)(first)
    pl.when(frame != 0)(second)


def send(level, piece, source, forward, backward, sems, columns=None):
    def start(targets):
        target = targets[level] if columns is None else targets[level].at[:, :, columns]
        return lambda: pltpu.make_async_copy(source, target, sems.at[piece]).start()

    by_frame(start(forward), start(backward))


def blank_kernel(features_ref, own_ref, *refs):
    outs, (*blanks, sems, own_sem) = refs[: 2 * LEVELS], refs[2 * LEVELS :]
    forward, backward = outs[:LEVELS], outs[LEVELS:]
    fetch = pltpu.make_async_copy(features_ref, own_ref, own_sem)
    fetch.start()
    for level, blank in enumerate(blanks):
        blank[...] = jnp.zeros_like(blank)
        send(level, level, blank, backward, forward, sems)
    for level, blank in enumerate(blanks):
        pltpu.make_async_copy(blank, backward[level], sems.at[level]).wait()
    fetch.wait()


def place_of(origin):
    pix = lax.axis_index("pix")
    return sum(jnp.where(pix == q, p, 0) for q, p in enumerate(origin))


def paired(line, summed, breadth):
    parts = []
    for c in range(line.shape[1] // LANES):
        summed[c, :breadth, :] = line[:, c * LANES : (c + 1) * LANES]
    for c in range(line.shape[1] // LANES):
        even = summed[c, pl.ds(0, breadth // 2, stride=2), :]
        odd = summed[c, pl.ds(1, breadth // 2, stride=2), :]
        parts.append((even + odd) * 0.25)
    return jnp.concatenate(parts, axis=1)


def level1_of(shard_ref, summed, breadth):
    upper = shard_ref[:breadth, :].astype(jnp.float32)
    return paired(upper + shard_ref[breadth : 2 * breadth, :].astype(jnp.float32), summed, breadth)


def split(value):
    high = value.astype(jnp.bfloat16)
    return high, (value - high.astype(jnp.float32)).astype(jnp.bfloat16)


def early_kernel(pix_count, breadth, own_ref, *refs):
    origins = origins_of(pix_count)
    count = len(origins) - 1
    shards, (scores_ref, partner_ref, high_ref, low_ref, partner1_ref, level2_ref) = refs[:count], refs[count : count + 6]
    target, level1, *summed = refs[count + 6 :]
    shard = own_ref.shape[0]
    half = breadth // 2
    last = place_of(origins[-1])
    far = 1 - last // 2
    factor = 1.0 / math.sqrt(own_ref.shape[1])
    for i, ref in enumerate(shards):
        place = place_of(origins[i])
        target[pl.ds(pl.multiple_of(place * shard, shard), shard), :] = ref[...]
        means = level1_of(ref, summed[i], breadth)
        at = pl.ds(pl.multiple_of(place * half, half), half)
        level1[at, :] = means
        high_ref[at, :], low_ref[at, :] = split(means)
    pair = target[pl.ds(pl.multiple_of(far * 2 * shard, 2 * shard), 2 * shard), :]
    scores = (dot_nt(own_ref[...], pair) * factor).astype(scores_ref.dtype)
    for r in range(2):
        scores_ref[r] = scores[r * breadth : (r + 1) * breadth, :]
    partner = last + 1 - 2 * (last % 2)
    partner_ref[...] = target[pl.ds(pl.multiple_of(partner * shard, shard), shard), :]
    partner1_ref[...] = level1[pl.ds(pl.multiple_of(partner * half, half), half), :]
    upper = level1[pl.ds(pl.multiple_of(far * breadth, half), half), :]
    lower = level1[pl.ds(pl.multiple_of(far * breadth + half, half), half), :]
    level2_ref[...] = paired(upper + lower, summed[0], half)


def late_kernel(pix_count, breadth, *refs):
    own_ref, relayed_ref, scores_ref, partner_ref, high_ref, low_ref, partner1_ref, far2_ref = refs[:8]
    outs, (target, highs, lows, level2, level3, summed, near_scores, v1, v2, v3, sems) = refs[8 + 2 * LEVELS : 8 + 4 * LEVELS], refs[8 + 4 * LEVELS :]
    forward, backward = outs[:LEVELS], outs[LEVELS:]
    shard = own_ref.shape[0]
    half, quarter = breadth // 2, breadth // 4
    last = place_of(origins_of(pix_count)[-1])
    near = last // 2
    far = 1 - near
    factor = 1.0 / math.sqrt(own_ref.shape[1])

    def columns(pair):
        return pl.ds(pl.multiple_of(pair * 2 * shard, 2 * shard), 2 * shard)

    send(0, LEVELS, scores_ref, forward, backward, sems, columns(far))
    odd = last % 2
    target[pl.ds(pl.multiple_of(odd * shard, shard), shard), :] = relayed_ref[...]
    target[pl.ds(pl.multiple_of((1 - odd) * shard, shard), shard), :] = partner_ref[...]
    own = own_ref[...]
    scores = (dot_nt(own, target[...]) * factor).astype(near_scores.dtype)
    for r in range(2):
        near_scores[r] = scores[r * breadth : (r + 1) * breadth, :]
    send(0, 0, near_scores, forward, backward, sems, columns(near))
    level1 = level1_of(relayed_ref, summed, breadth)
    highs[...] = high_ref[...]
    lows[...] = low_ref[...]
    at = pl.ds(pl.multiple_of(last * half, half), half)
    highs[at, :], lows[at, :] = split(level1)
    level2[pl.ds(pl.multiple_of(near * quarter, quarter), quarter), :] = paired(level1 + partner1_ref[...], summed, half)
    level2[pl.ds(pl.multiple_of(far * quarter, quarter), quarter), :] = far2_ref[...]
    eighth = quarter // 2
    level3[...] = jnp.zeros_like(level3)
    level3[:eighth, :] = paired(level2[:quarter, :] + level2[quarter:, :], summed, quarter)
    halves = ((dot_nt(own, highs[...]) + dot_nt(own, lows[...])) * factor).astype(v1.dtype)
    high, low = split(jnp.concatenate([level2[...], level3[...]], axis=0))
    lines = []
    for r in range(2):
        v1[r] = halves[r * breadth : (r + 1) * breadth, :]
        mine = own[r * breadth : (r + 1) * breadth, :]
        product = (dot_nt(high, mine) + dot_nt(low, mine)) * factor
        v2[r] = product[:half, :].astype(v2.dtype)
        lines.append(product[half : half + eighth, :])
    v3[...] = jnp.stack(lines, axis=1).astype(v3.dtype)

    def start(targets):
        def run():
            for level, value in ((1, v1), (2, v2), (3, v3)):
                pltpu.make_async_copy(value, targets[level], sems.at[level]).start()

        return run

    by_frame(start(forward), start(backward))
    pltpu.make_async_copy(scores_ref, forward[0].at[:, :, columns(far)], sems.at[LEVELS]).wait()
    pltpu.make_async_copy(near_scores, forward[0].at[:, :, columns(near)], sems.at[0]).wait()
    for level, value in ((1, v1), (2, v2), (3, v3)):
        pltpu.make_async_copy(value, forward[level], sems.at[level]).wait()


ROUNDS = ((2, 0, 3, 1), (1, 3, 0, 2), (0, 2, 1, 3))


def origins_of(pix_count):
    origins = [[row.index(q) for q in range(pix_count)] for row in ROUNDS]
    return origins + [[ROUNDS[0].index(q ^ 1) for q in range(pix_count)]]


def exchange(own, pix_count):
    got = []
    for row in ROUNDS:
        pairs = [(f * pix_count + p, (1 - f) * pix_count + row[p]) for f in range(2) for p in range(pix_count)]
        got.append(lax.ppermute(own, ("frame", "pix"), pairs))
    got.append(lax.ppermute(got[0], "pix", [(p, p ^ 1) for p in range(pix_count)]))
    return got


def two_frames(features):
    rows, breadth, channels = features.shape[1:]
    pix_count = lax.axis_size("pix")
    shard = rows * breadth
    pixels = shard * pix_count
    own = features.reshape(shard, channels)
    *direct, relayed = exchange(own, pix_count)

    shapes = [
        (rows, breadth, pixels),
        (rows, breadth, pixels // 4),
        (rows, pixels // 16, breadth),
        (pixels // 64, rows, breadth),
    ]
    vmem = pl.BlockSpec(memory_space=pltpu.VMEM)
    anywhere = pl.BlockSpec(memory_space=pl.ANY)
    hbm = pl.BlockSpec(memory_space=pltpu.HBM)
    out_shapes = [jax.ShapeDtypeStruct(s, jnp.bfloat16) for s in shapes * 2]
    limits = pltpu.CompilerParams(vmem_limit_bytes=12 * 2**20)

    def cost(flops):
        return pl.CostEstimate(flops=flops, bytes_accessed=4 * shard * pixels, transcendentals=0)

    def scratch(kind, *shape):
        return pltpu.VMEM(shape, kind)

    flops = shard * pixels * channels
    near, *blanks = pl.pallas_call(
        blank_kernel,
        out_shape=[jax.ShapeDtypeStruct(own.shape, own.dtype)] + out_shapes,
        in_specs=[hbm],
        out_specs=[vmem] + [anywhere] * (2 * LEVELS),
        scratch_shapes=[scratch(jnp.bfloat16, *s) for s in shapes]
        + [pltpu.SemaphoreType.DMA((LEVELS,)), pltpu.SemaphoreType.DMA],
        compiler_params=limits,
        cost_estimate=cost(flops),
    )(own)
    early = pl.pallas_call(
        functools.partial(early_kernel, pix_count, breadth),
        out_shape=[
            jax.ShapeDtypeStruct((rows, breadth, 2 * shard), jnp.bfloat16),
            jax.ShapeDtypeStruct((shard, channels), jnp.bfloat16),
            jax.ShapeDtypeStruct((pixels // 4, channels), jnp.bfloat16),
            jax.ShapeDtypeStruct((pixels // 4, channels), jnp.bfloat16),
            jax.ShapeDtypeStruct((shard // 4, channels), jnp.float32),
            jax.ShapeDtypeStruct((shard // 8, channels), jnp.float32),
        ],
        in_specs=[vmem] * (1 + len(direct)),
        out_specs=[vmem] * 6,
        scratch_shapes=[
            scratch(jnp.bfloat16, pixels, channels),
            scratch(jnp.float32, pixels // 4, channels),
        ]
        + [scratch(jnp.float32, channels // LANES, breadth, LANES)] * len(direct),
        compiler_params=limits,
        cost_estimate=cost(2 * flops),
    )(near, *direct)
    outs = pl.pallas_call(
        functools.partial(late_kernel, pix_count, breadth),
        out_shape=out_shapes,
        in_specs=[vmem] * 8 + [anywhere] * (2 * LEVELS),
        out_specs=[anywhere] * (2 * LEVELS),
        scratch_shapes=[
            scratch(jnp.bfloat16, 2 * shard, channels),
            scratch(jnp.bfloat16, pixels // 4, channels),
            scratch(jnp.bfloat16, pixels // 4, channels),
            scratch(jnp.float32, pixels // 16, channels),
            scratch(jnp.float32, -(-pixels // 64 // 16) * 16, channels),
            scratch(jnp.float32, channels // LANES, breadth, LANES),
            scratch(jnp.bfloat16, rows, breadth, 2 * shard),
        ]
        + [scratch(jnp.bfloat16, *s) for s in shapes[1:]]
        + [pltpu.SemaphoreType.DMA((LEVELS + 1,))],
        input_output_aliases={8 + i: i for i in range(2 * LEVELS)},
        compiler_params=limits,
        cost_estimate=cost(2 * flops),
    )(near, relayed, *early, *blanks)
    result = []
    for d in range(2):
        full, half, quarter, eighth = outs[d * LEVELS : (d + 1) * LEVELS]
        result += [full[None], half[None], jnp.transpose(quarter, (0, 2, 1))[None], jnp.transpose(eighth, (1, 2, 0))[None]]
    return tuple(result)


def per_device(frame_count, pix_count, features):
    rows, breadth, channels = features.shape[1:]
    fits = frame_count == 2 and pix_count == len(ROUNDS) + 1 and rows == 2 and breadth % 32 == 0 and channels % LANES == 0
    return two_frames(features) if fits and 2 * rows * breadth % LANES == 0 else many_frames(features)


def solution(mesh):
    spec = P(("clip", "frame"), "pix", None, None)

    def body(features):
        return per_device(mesh.shape["frame"], mesh.shape["pix"], features)

    return jax.shard_map(
        body, mesh=mesh, in_specs=(spec,), out_specs=(spec,) * (2 * LEVELS), check_vma=False
    )
```
